16 devices in a mesh: pp: 2 (over z), ep: 8 (over y, x, core).
Axes of the slice: x: 2, y: 2, z: 2, core: 2. Of those that a mesh axis runs over, the one named last changes fastest.
Arguments:
- x_f: bfloat16 [2, 16384, 512], P('pp', 'ep')
- pos_f: int32 [2, 16384, 6], P('pp', 'ep')
- gate_f: bfloat16 [2, 16384, 6], P('pp', 'ep')
- x_b: bfloat16 [2, 16384, 512], P('pp', 'ep')
- dy_b: bfloat16 [2, 16384, 512], P('pp', 'ep')
- pos_b: int32 [2, 16384, 6], P('pp', 'ep')
- gate_b: bfloat16 [2, 16384, 6], P('pp', 'ep')
- xe_b: bfloat16 [2, 8, 64, 384, 512], P('pp', None, 'ep')
- w_in: bfloat16 [2, 512, 2816], P('pp')
- w_out: bfloat16 [2, 2816, 512], P('pp')
- ws_gate: bfloat16 [2, 512, 768], P('pp')
- ws_up: bfloat16 [2, 512, 768], P('pp')
- ws_down: bfloat16 [2, 768, 512], P('pp')
- we_gate: bfloat16 [2, 64, 512, 384], P('pp', 'ep')
- we_up: bfloat16 [2, 64, 512, 384], P('pp', 'ep')
- we_down: bfloat16 [2, 64, 384, 512], P('pp', 'ep')
Outputs:
- output 1: bfloat16 [2, 16384, 512], P('pp', 'ep')
- output 2: bfloat16 [2, 16384, 512], P('pp', 'ep')
- output 3: float32 [2, 64, 512, 384], P('pp', 'ep')
- output 4: float32 [2, 64, 512, 384], P('pp', 'ep')
- output 5: float32 [2, 64, 384, 512], P('pp', 'ep')
All inputs are finite; a program needn't handle non-finite values.
Results may differ from the reference program's by a relative error of at most 0.00963231.
Values are sent between devices in bfloat16 or wider.
A program may use at most 1 GiB of HBM per device.

```python
import jax
import jax.numpy as jnp
from jax import lax

STAGES = 2
GROUP = 8
TOK = 2048
D = 512
FD = 2816
FS = 768
FE = 384
EXPERTS = 64
TOP = 6
CAP = 2 * TOK * TOP // EXPERTS
N_SLOTS = EXPERTS * CAP
EPS = 1e-6


def rms_norm(x_val):
    x_f32 = x_val.astype(jnp.float32)
    inv_rms = lax.rsqrt(jnp.mean(x_f32 * x_f32, axis=-1, keepdims=True) + EPS)
    return (x_f32 * inv_rms).astype(jnp.bfloat16), inv_rms


def rms_back(x_val, inv_rms, d_norm):
    x_f32 = x_val.astype(jnp.float32)
    proj_mean = jnp.mean(d_norm * x_f32, axis=-1, keepdims=True)
    return inv_rms * d_norm - x_f32 * (inv_rms * inv_rms * inv_rms) * proj_mean


def silu_grad(pre_val):
    sig_val = jax.nn.sigmoid(pre_val)
    return sig_val * (1.0 + pre_val * (1.0 - sig_val))


def dense_fwd(x_val, w_in, w_out):
    normed, inv_in = rms_norm(x_val)
    pre_act = jnp.dot(normed, w_in, preferred_element_type=jnp.float32)
    dense_act = jax.nn.silu(pre_act).astype(jnp.bfloat16)
    mlp_out = jnp.dot(dense_act, w_out, preferred_element_type=jnp.float32)
    hidden = (x_val.astype(jnp.float32) + mlp_out).astype(jnp.bfloat16)
    return hidden, inv_in, pre_act


def shared_fwd(normed, ws_gate, ws_up, ws_down):
    gate_pre = jnp.dot(normed, ws_gate, preferred_element_type=jnp.float32)
    up_pre = jnp.dot(normed, ws_up, preferred_element_type=jnp.float32)
    glu_act = (jax.nn.silu(gate_pre) * up_pre).astype(jnp.bfloat16)
    return jnp.dot(glu_act, ws_down, preferred_element_type=jnp.float32)


def shared_back(normed, d_out, ws_gate, ws_up, ws_down):
    gate_pre = jnp.dot(normed, ws_gate, preferred_element_type=jnp.float32)
    up_pre = jnp.dot(normed, ws_up, preferred_element_type=jnp.float32)
    d_act = jnp.dot(d_out, ws_down.T, preferred_element_type=jnp.float32)
    d_gate = (d_act * up_pre * silu_grad(gate_pre)).astype(jnp.bfloat16)
    d_up = (d_act * jax.nn.silu(gate_pre)).astype(jnp.bfloat16)
    return jnp.dot(d_gate, ws_gate.T, preferred_element_type=jnp.float32) + jnp.dot(d_up, ws_up.T, preferred_element_type=jnp.float32)


def expert_fwd(buf_rows, we_gate, we_up, we_down):
    rows_f32 = buf_rows.astype(jnp.float32)
    gate_pre = jnp.einsum('sech,ehf->secf', rows_f32, we_gate.astype(jnp.float32))
    up_pre = jnp.einsum('sech,ehf->secf', rows_f32, we_up.astype(jnp.float32))
    glu_act = (jax.nn.silu(gate_pre) * up_pre).astype(jnp.bfloat16)
    return jnp.einsum('secf,efh->sech', glu_act.astype(jnp.float32), we_down.astype(jnp.float32)).astype(jnp.bfloat16)


def expert_back(buf_rows, d_out, we_gate, we_up, we_down):
    rows_f32 = buf_rows.astype(jnp.float32)
    d_out_f32 = d_out.astype(jnp.float32)
    gate_f32 = we_gate.astype(jnp.float32)
    up_f32 = we_up.astype(jnp.float32)
    gate_pre = jnp.einsum('sech,ehf->secf', rows_f32, gate_f32)
    up_pre = jnp.einsum('sech,ehf->secf', rows_f32, up_f32)
    gate_act = jax.nn.silu(gate_pre)
    glu_act = (gate_act * up_pre).astype(jnp.bfloat16).astype(jnp.float32)
    d_wd = jnp.einsum('secf,sech->efh', glu_act, d_out_f32)
    d_act = jnp.einsum('sech,efh->secf', d_out_f32, we_down.astype(jnp.float32))
    d_gate = (d_act * up_pre * silu_grad(gate_pre)).astype(jnp.bfloat16).astype(jnp.float32)
    d_up = (d_act * gate_act).astype(jnp.bfloat16).astype(jnp.float32)
    d_wg = jnp.einsum('sech,secf->ehf', rows_f32, d_gate)
    d_wu = jnp.einsum('sech,secf->ehf', rows_f32, d_up)
    d_rows = (jnp.einsum('secf,ehf->sech', d_gate, gate_f32) + jnp.einsum('secf,ehf->sech', d_up, up_f32)).astype(jnp.bfloat16)
    return d_rows, d_wg, d_wu, d_wd


def spread_rows(normed):
    return jnp.broadcast_to(normed.reshape(GROUP, TOK, 1, D), (GROUP, TOK, TOP, D)).reshape(GROUP, TOK * TOP, D)


def scatter_rows(route_rows, route_pos):
    flat_pos = route_pos.reshape(GROUP, TOK * TOP)

    def scatter_one(row_blk, pos_blk):
        return jnp.zeros((N_SLOTS, D), row_blk.dtype).at[pos_blk].set(row_blk)

    return jax.vmap(scatter_one)(route_rows, flat_pos).reshape(GROUP, EXPERTS, CAP, D)


def gather_rows(buffers, route_pos):
    flat_buf = buffers.reshape(GROUP, N_SLOTS, D)
    flat_pos = route_pos.reshape(GROUP, TOK * TOP)
    picked = jax.vmap(lambda buf_blk, pos_blk: jnp.take(buf_blk, pos_blk, axis=0))(flat_buf, flat_pos)
    return picked.reshape(GROUP * TOK, TOP, D)


def stage_slot(stage_args):
    (x_f, pos_f, gate_f, x_b, dy_b, pos_b, gate_b, xe_b, w_in, w_out, ws_gate, ws_up, ws_down, we_gate, we_up, we_down) = stage_args
    hidden, _, _ = dense_fwd(x_f, w_in, w_out)
    normed, _ = rms_norm(hidden)
    shared = shared_fwd(normed, ws_gate, ws_up, ws_down)
    exp_out = expert_fwd(scatter_rows(spread_rows(normed), pos_f), we_gate, we_up, we_down)
    picked = gather_rows(exp_out, pos_f)
    routed = jnp.einsum('tk,tkd->td', gate_f.astype(jnp.float32), picked.astype(jnp.float32))
    y_out = (hidden.astype(jnp.float32) + shared + routed).astype(jnp.bfloat16)

    hidden_b, inv_in, pre_act = dense_fwd(x_b, w_in, w_out)
    normed_b, inv_mid = rms_norm(hidden_b)
    dy_f32 = dy_b.astype(jnp.float32)
    d_routes = (gate_b.astype(jnp.float32)[:, :, None] * dy_f32[:, None, :]).astype(jnp.bfloat16)
    d_buf = scatter_rows(d_routes.reshape(GROUP, TOK * TOP, D), pos_b)
    d_rows, d_wg, d_wu, d_wd = expert_back(xe_b, d_buf, we_gate, we_up, we_down)
    d_picked = gather_rows(d_rows, pos_b)
    d_norm = shared_back(normed_b, dy_b, ws_gate, ws_up, ws_down) + jnp.sum(d_picked.astype(jnp.float32), axis=1)
    d_hidden = dy_f32 + rms_back(hidden_b, inv_mid, d_norm)
    d_act = jnp.dot(d_hidden.astype(jnp.bfloat16), w_out.T, preferred_element_type=jnp.float32)
    d_pre = (d_act * silu_grad(pre_act)).astype(jnp.bfloat16)
    d_in = jnp.dot(d_pre, w_in.T, preferred_element_type=jnp.float32)
    d_x = (d_hidden + rms_back(x_b, inv_in, d_in)).astype(jnp.bfloat16)
    return y_out, d_x, d_wg, d_wu, d_wd


def draw_routes(route_key):
    avg_count = TOK * TOP // EXPERTS
    key_order, key_shift, key_perm = jax.random.split(route_key, 3)
    exp_order = jax.random.permutation(key_order, EXPERTS)
    pair_shift = jax.random.randint(key_shift, (EXPERTS // 2,), 0, avg_count + 1)
    pair_shift = pair_shift.at[0].set(avg_count)
    paired = jnp.stack([avg_count + pair_shift, avg_count - pair_shift], axis=1).reshape(EXPERTS).astype(jnp.int32)
    counts = jnp.zeros((EXPERTS,), jnp.int32).at[exp_order].set(paired)
    count_ends = jnp.cumsum(counts).astype(jnp.int32)
    route_ids = jnp.arange(TOK * TOP, dtype=jnp.int32)
    expert_of = jnp.searchsorted(count_ends, route_ids, side='right').astype(jnp.int32)
    slot_of = route_ids - (count_ends - counts)[expert_of]
    flat_pos = expert_of * CAP + slot_of
    route_perm = jax.random.permutation(key_perm, TOK * TOP)
    return flat_pos[route_perm].reshape(TOK, TOP)


def draw_all_routes(route_key):
    return jax.vmap(draw_routes)(jax.random.split(route_key, STAGES * GROUP)).reshape(STAGES, GROUP * TOK, TOP)


def saved_rows(x_b, pos_b, w_in, w_out):
    def stage_rows(stage_args):
        x_val, pos_val, w_first, w_second = stage_args
        hidden, _, _ = dense_fwd(x_val, w_first, w_second)
        normed, _ = rms_norm(hidden)
        return scatter_rows(spread_rows(normed), pos_val)

    return lax.map(stage_rows, (x_b, pos_b, w_in, w_out))


def normal_weight(w_key, w_shape, fan_in, w_gain):
    return (jax.random.normal(w_key, w_shape, jnp.float32) * (w_gain * fan_in ** -0.5)).astype(jnp.bfloat16)


def setup_inputs(seed: int = 0) -> dict:
    key_list = jax.random.split(jax.random.key(seed), 16)
    tok_shape = (STAGES, GROUP * TOK, D)
    route_shape = (STAGES, GROUP * TOK, TOP)
    x_f = jax.random.normal(key_list[0], tok_shape, jnp.float32).astype(jnp.bfloat16)
    pos_f = draw_all_routes(key_list[1])
    gate_f = (jax.random.uniform(key_list[2], route_shape, jnp.float32, 0.5, 1.5) * TOP ** -0.5).astype(jnp.bfloat16)
    x_b = jax.random.normal(key_list[3], tok_shape, jnp.float32).astype(jnp.bfloat16)
    dy_b = jax.random.normal(key_list[4], tok_shape, jnp.float32).astype(jnp.bfloat16)
    pos_b = draw_all_routes(key_list[5])
    gate_b = (jax.random.uniform(key_list[6], route_shape, jnp.float32, 0.5, 1.5) * TOP ** -0.5).astype(jnp.bfloat16)
    w_in = normal_weight(key_list[7], (STAGES, D, FD), D, 1.0)
    w_out = normal_weight(key_list[8], (STAGES, FD, D), FD, 1.0)
    ws_gate = normal_weight(key_list[9], (STAGES, D, FS), D, 1.0)
    ws_up = normal_weight(key_list[10], (STAGES, D, FS), D, 1.0)
    ws_down = normal_weight(key_list[11], (STAGES, FS, D), FS, 1.0)
    we_gate = normal_weight(key_list[12], (STAGES, EXPERTS, D, FE), D, 1.0)
    we_up = normal_weight(key_list[13], (STAGES, EXPERTS, D, FE), D, 1.0)
    we_down = normal_weight(key_list[14], (STAGES, EXPERTS, FE, D), FE, 1.5)
    xe_b = saved_rows(x_b, pos_b, w_in, w_out)
    return {'x_f': x_f, 'pos_f': pos_f, 'gate_f': gate_f, 'x_b': x_b, 'dy_b': dy_b, 'pos_b': pos_b, 'gate_b': gate_b, 'xe_b': xe_b, 'w_in': w_in, 'w_out': w_out, 'ws_gate': ws_gate, 'ws_up': ws_up, 'ws_down': ws_down, 'we_gate': we_gate, 'we_up': we_up, 'we_down': we_down}


def reference(x_f, pos_f, gate_f, x_b, dy_b, pos_b, gate_b, xe_b, w_in, w_out, ws_gate, ws_up, ws_down, we_gate, we_up, we_down):
    y_out, d_x, d_wg, d_wu, d_wd = lax.map(stage_slot, (x_f, pos_f, gate_f, x_b, dy_b, pos_b, gate_b, xe_b, w_in, w_out, ws_gate, ws_up, ws_down, we_gate, we_up, we_down))
    return jnp.roll(y_out, 1, axis=0), jnp.roll(d_x, -1, axis=0), d_wg, d_wu, d_wd
```

```python
import functools

import jax
import jax.numpy as jnp
from jax import lax
from jax.experimental import pallas as pl
from jax.experimental.layout import Layout, with_layout_constraint
from jax.experimental.pallas import tpu as pltpu
from jax.sharding import PartitionSpec as P

EPS = 1e-6
LANES = 128
BLK = 64
CHUNK = 512 // BLK
F32 = jnp.float32
BF16 = jnp.bfloat16


def rms_norm(x_val):
    x_f32 = x_val.astype(F32)
    inv_rms = lax.rsqrt(jnp.mean(x_f32 * x_f32, axis=-1, keepdims=True) + EPS)
    return (x_f32 * inv_rms).astype(BF16), inv_rms


def rms_back(x_val, inv_rms, d_norm):
    x_f32 = x_val.astype(F32)
    proj_mean = jnp.mean(d_norm * x_f32, axis=-1, keepdims=True)
    return inv_rms * d_norm - x_f32 * (inv_rms * inv_rms * inv_rms) * proj_mean


def silu_grad(pre_val):
    sig_val = jax.nn.sigmoid(pre_val)
    return sig_val * (1.0 + pre_val * (1.0 - sig_val))


def dense_fwd(x_val, w_in, w_out):
    normed, inv_in = rms_norm(x_val)
    pre_act = jnp.dot(normed, w_in, preferred_element_type=F32)
    dense_act = jax.nn.silu(pre_act).astype(BF16)
    mlp_out = jnp.dot(dense_act, w_out, preferred_element_type=F32)
    return (x_val.astype(F32) + mlp_out).astype(BF16), inv_in, pre_act


def dense_back(d_hidden, x_val, inv_in, pre_act, w_in, w_out):
    d_act = jnp.einsum('th,fh->tf', d_hidden.astype(BF16), w_out, preferred_element_type=F32)
    d_pre = (d_act * silu_grad(pre_act)).astype(BF16)
    d_in = jnp.einsum('tf,hf->th', d_pre, w_in, preferred_element_type=F32)
    return (d_hidden + rms_back(x_val, inv_in, d_in)).astype(BF16)


def shared_fwd(normed, ws_gate, ws_up, ws_down):
    gate_pre = jnp.dot(normed, ws_gate, preferred_element_type=F32)
    up_pre = jnp.dot(normed, ws_up, preferred_element_type=F32)
    glu_act = (jax.nn.silu(gate_pre) * up_pre).astype(BF16)
    return jnp.dot(glu_act, ws_down, preferred_element_type=F32)


def shared_back(normed, d_out, ws_gate, ws_up, ws_down):
    gate_pre = jnp.dot(normed, ws_gate, preferred_element_type=F32)
    up_pre = jnp.dot(normed, ws_up, preferred_element_type=F32)
    d_act = jnp.einsum('th,fh->tf', d_out, ws_down, preferred_element_type=F32)
    d_gate = (d_act * up_pre * silu_grad(gate_pre)).astype(BF16)
    d_up = (d_act * jax.nn.silu(gate_pre)).astype(BF16)
    return jnp.einsum('tf,hf->th', d_gate, ws_gate, preferred_element_type=F32) + jnp.einsum('tf,hf->th', d_up, ws_up, preferred_element_type=F32)


def iota_f32(shape, dim):
    return lax.broadcasted_iota(jnp.int32, shape, dim).astype(F32)


def compile_args(flops, n_bytes, vmem_mib=56):
    return dict(
        compiler_params=pltpu.CompilerParams(
            dimension_semantics=('arbitrary',), vmem_limit_bytes=vmem_mib * 1024 * 1024),
        cost_estimate=pl.CostEstimate(flops=int(flops), bytes_accessed=int(n_bytes), transcendentals=0))


def route_maps(pos_pair, gate_pair, n_group, n_rows):
    n_set, n_top, n_tok = pos_pair.shape
    n_hi = n_group * n_rows

    def kernel(pos_ref, gate_ref, out_ref):
        tok_row = lax.broadcasted_iota(jnp.int32, (1, n_tok), 1) + 1
        tok_hi = (tok_row >> 6).astype(F32)
        tok_lo = (tok_row & 63).astype(F32)
        hi_iota = lax.broadcasted_iota(jnp.int32, (n_hi, n_tok), 0)
        lo_iota = lax.broadcasted_iota(jnp.int32, (LANES, n_tok), 0)
        for set_idx in range(n_set):
            def add_route(rank, total):
                pos_row = pos_ref[set_idx, pl.ds(rank, 1), :]
                gate_row = gate_ref[set_idx, pl.ds(rank, 1), :]
                hi_hot = jnp.where(hi_iota == (pos_row >> 7), 1.0, 0.0).astype(BF16)
                lo_eq = lo_iota == (pos_row & (LANES - 1))
                rhs = jnp.concatenate([jnp.where(lo_eq, val, 0.0).astype(BF16) for val in (tok_hi, tok_lo, gate_row)], axis=0)
                return total + lax.dot_general(hi_hot, rhs, (((1,), (1,)), ((), ())), preferred_element_type=F32)

            total = lax.fori_loop(0, n_top, add_route, jnp.zeros((n_hi, 3 * LANES), F32))
            tok_map = total[:, :LANES] * 64.0 + total[:, LANES:2 * LANES] - 1.0
            out_ref[:, 2 * set_idx] = tok_map.reshape(n_group, n_rows, LANES)
            out_ref[:, 2 * set_idx + 1] = total[:, 2 * LANES:].reshape(n_group, n_rows, LANES)

    return pl.pallas_call(
        kernel,
        out_shape=jax.ShapeDtypeStruct((n_group, 2 * n_set, n_rows, LANES), F32),
        compiler_params=pltpu.CompilerParams(vmem_limit_bytes=48 * 1024 * 1024),
        cost_estimate=pl.CostEstimate(flops=2 * n_set * n_top * n_tok * n_hi * 3 * LANES, bytes_accessed=2 ** 20, transcendentals=0),
    )(pos_pair, gate_pair)


def list_blocks(flag_at, list_ref, n_rows, pad_to):
    def step(idx, count):
        list_ref[count] = idx
        return count + flag_at(idx)

    count = lax.fori_loop(0, n_rows, step, jnp.int32(0))
    last = list_ref[jnp.maximum(count - 1, 0)]
    for extra in range(pad_to - 1):
        list_ref[count + extra] = last
    return count


def gather_rows(flags, maps, tok_plane, rows, gated, sources, after, into=None):
    n_group, n_rows = maps.shape[0], maps.shape[2]
    n_src, n_tok, d_model = rows.shape
    n_slots = n_rows * BLK
    n_part = CHUNK
    extra = tuple(after) + (() if into is None else (into,))

    def kernel(flag_ref, source_ref, tok_ref, gate_ref, row_ref, *refs):
        out_ref, list_ref = refs[-2:]
        src = source_ref[pl.program_id(0)]
        count = list_blocks(lambda idx: flag_ref[src * n_rows + idx], list_ref, n_rows, n_part)
        lane = iota_f32((BLK, LANES), 1)

        def columns(ref, idx):
            return jnp.transpose(jnp.broadcast_to(ref[0, 0, pl.ds(idx, 1), :], (LANES, LANES)))[:BLK]

        def chunk(step, carry):
            picks = []
            for entry in range(n_part):
                idx = list_ref[n_part * step + entry]
                tok_col = columns(tok_ref, idx)
                tok_hi = jnp.floor(tok_col * (1.0 / LANES))
                val = columns(gate_ref, idx) if gated else 1.0
                hot = jnp.where(tok_col - tok_hi * LANES == lane, val, 0.0).astype(BF16)
                tok_hi = tok_hi.astype(BF16)
                picks.append(jnp.concatenate(
                    [jnp.where(tok_hi == jnp.asarray(part, BF16), hot, jnp.zeros_like(hot)) for part in range(n_tok // LANES)], axis=1))
            picked = jnp.dot(jnp.concatenate(picks, axis=0), row_ref[0], preferred_element_type=F32).astype(BF16)
            for entry in range(n_part):
                idx = list_ref[n_part * step + entry]
                out_ref[0, pl.ds(pl.multiple_of(idx * BLK, BLK), BLK), :] = picked[entry * BLK:(entry + 1) * BLK]
            return carry

        lax.fori_loop(0, (count + n_part - 1) // n_part, chunk, 0)

    return pl.pallas_call(
        kernel,
        out_shape=jax.ShapeDtypeStruct((n_group, n_slots, d_model), BF16),
        grid_spec=pltpu.PrefetchScalarGridSpec(
            num_scalar_prefetch=2, grid=(n_src,),
            in_specs=[
                pl.BlockSpec((1, 1, n_rows, LANES), lambda s, f, o: (o[s], tok_plane, 0, 0)),
                pl.BlockSpec((1, 1, n_rows, LANES), lambda s, f, o: (o[s], tok_plane + 1, 0, 0)),
                pl.BlockSpec((1, n_tok, d_model), lambda s, f, o: (s, 0, 0)),
            ] + [pl.BlockSpec(memory_space=pl.ANY)] * len(extra),
            out_specs=pl.BlockSpec((1, n_slots, d_model), lambda s, f, o: (o[s], 0, 0)),
            scratch_shapes=[pltpu.SMEM((n_rows + 8,), jnp.int32)]),
        input_output_aliases={} if into is None else {4 + len(extra): 0},
        **compile_args(1.2 * n_src * n_slots * n_tok * d_model, n_src * (n_slots + n_tok) * d_model * 2),
    )(flags, sources, maps, maps, rows, *extra)


def combine_rows(flags, maps, tok_plane, rows, n_tok, gated, sources, after):
    n_group = sources.shape[0]
    n_slots, d_model = rows.shape[1:]
    n_rows = maps.shape[2]
    m_tile = 1024

    def kernel(flag_ref, source_ref, tok_ref, gate_ref, row_ref, *refs):
        out_ref, list_ref = refs[-2:]
        src = source_ref[pl.program_id(0)]
        count = list_blocks(lambda idx: flag_ref[src * n_rows + idx], list_ref, n_rows, CHUNK)
        out_ref[...] = jnp.zeros_like(out_ref)
        tok_iota = iota_f32((LANES, LANES), 0)
        low_lanes = lax.broadcasted_iota(jnp.int32, (1, LANES), 1) < BLK

        def chunk(step, carry):
            toks, vals, parts = [], [], []
            for entry in range(CHUNK):
                idx = list_ref[CHUNK * step + entry]
                toks.append(jnp.where(CHUNK * step + entry < count, tok_ref[0, 0, pl.ds(idx, 1), :], -1.0))
                vals.append(gate_ref[0, 0, pl.ds(idx, 1), :] if gated else 1.0)
                parts.append(row_ref[0, pl.ds(pl.multiple_of(idx * BLK, BLK), BLK), :])
            toks = [jnp.where(low_lanes, *toks[2 * part:2 * part + 2]) for part in range(CHUNK // 2)]
            hots, his = [], []
            for part in range(CHUNK // 2):
                val = jnp.where(low_lanes, *vals[2 * part:2 * part + 2]) if gated else 1.0
                tok_hi = jnp.floor(toks[part] * (1.0 / LANES))
                hots.append(jnp.where(tok_iota == toks[part] - tok_hi * LANES, val, 0.0).astype(BF16))
                his.append(jnp.broadcast_to(tok_hi, (LANES, LANES)).astype(BF16))
            row_chunk = jnp.concatenate(parts, axis=0)
            for m_idx in range(n_tok // m_tile):
                weights = jnp.concatenate([jnp.concatenate(
                    [jnp.where(hi == jnp.asarray(sub, BF16), hot, jnp.zeros_like(hot)) for sub in range(m_idx * m_tile // LANES, (m_idx + 1) * m_tile // LANES)],
                    axis=0) for hot, hi in zip(hots, his)], axis=1)
                out_ref[0, m_idx * m_tile:(m_idx + 1) * m_tile, :] += jnp.dot(weights, row_chunk, preferred_element_type=F32)
            return carry

        lax.fori_loop(0, (count + CHUNK - 1) // CHUNK, chunk, 0)

    return pl.pallas_call(
        kernel,
        out_shape=jax.ShapeDtypeStruct((n_group, n_tok, d_model), F32),
        grid_spec=pltpu.PrefetchScalarGridSpec(
            num_scalar_prefetch=2, grid=(n_group,),
            in_specs=[
                pl.BlockSpec((1, 1, n_rows, LANES), lambda s, f, o: (o[s], tok_plane, 0, 0)),
                pl.BlockSpec((1, 1, n_rows, LANES), lambda s, f, o: (o[s], tok_plane + 1, 0, 0)),
                pl.BlockSpec((1, n_slots, d_model), lambda s, f, o: (o[s], 0, 0)),
            ] + [pl.BlockSpec(memory_space=pl.ANY)] * len(after),
            out_specs=pl.BlockSpec((1, n_tok, d_model), lambda s, f, o: (s, 0, 0)),
            scratch_shapes=[pltpu.SMEM((n_rows + 8,), jnp.int32)]),
        **compile_args(1.2 * n_group * n_slots * n_tok * d_model, n_group * (n_slots * 2 + n_tok * 4) * d_model),
    )(flags, sources, maps, maps, rows, *after)


def expert_fwd(flags, rows, w_gu, w_down):
    n_group, n_exp, n_cap, d_model = rows.shape
    d_exp = w_down.shape[1]
    n_blk = n_cap // BLK
    n_rows = n_exp * n_blk

    def kernel(flag_ref, row_ref, gu_ref, down_ref, out_ref, list_ref):
        exp_idx = pl.program_id(0)
        flag_at = lambda idx: flag_ref[(idx // n_blk) * n_rows + exp_idx * n_blk + idx % n_blk]
        count = list_blocks(flag_at, list_ref, n_group * n_blk, CHUNK)

        def chunk(step, carry):
            where_at = []
            for half in range(CHUNK):
                idx = list_ref[CHUNK * step + half]
                where_at.append((idx // n_blk, pl.ds(pl.multiple_of((idx % n_blk) * BLK, BLK), BLK)))
            x_val = jnp.concatenate([row_ref[s, 0, rng, :] for s, rng in where_at], axis=0)
            pre = jnp.dot(x_val, gu_ref[0], preferred_element_type=F32)
            act = (jax.nn.silu(pre[:, :d_exp]) * pre[:, d_exp:]).astype(BF16)
            out = jnp.dot(act, down_ref[0], preferred_element_type=F32).astype(BF16)
            for half, (s, rng) in enumerate(where_at):
                out_ref[s, 0, rng, :] = out[half * BLK:(half + 1) * BLK]
            return carry

        lax.fori_loop(0, (count + CHUNK - 1) // CHUNK, chunk, 0)

    row_spec = pl.BlockSpec((n_group, 1, n_cap, d_model), lambda e, f: (0, e, 0, 0))
    return pl.pallas_call(
        kernel,
        out_shape=jax.ShapeDtypeStruct(rows.shape, BF16),
        grid_spec=pltpu.PrefetchScalarGridSpec(
            num_scalar_prefetch=1, grid=(n_exp,),
            in_specs=[row_spec,
                      pl.BlockSpec((1, d_model, 2 * d_exp), lambda e, f: (e, 0, 0)),
                      pl.BlockSpec((1, d_exp, d_model), lambda e, f: (e, 0, 0))],
            out_specs=row_spec,
            scratch_shapes=[pltpu.SMEM((n_group * n_blk + 8,), jnp.int32)]),
        **compile_args(1.4 * n_group * n_exp * n_cap * d_model * d_exp * 3, n_group * n_exp * n_cap * d_model * 4),
    )(flags, rows, w_gu, w_down)


def expert_back(flags, rows, d_out, w_gu, w_gu_t, w_down_t):
    n_group, n_exp, n_cap, d_model = rows.shape
    d_exp = w_down_t.shape[2]
    n_blk = n_cap // BLK
    n_rows = n_exp * n_blk

    def kernel(flag_ref, row_ref, dout_ref, gu_ref, gut_ref, dnt_ref, dx_ref, dwg_ref, dwu_ref, dwd_ref, list_ref):
        exp_idx = pl.program_id(0)
        flag_at = lambda idx: flag_ref[(idx // n_blk) * n_rows + exp_idx * n_blk + idx % n_blk]
        count = list_blocks(flag_at, list_ref, n_group * n_blk, CHUNK)
        dwg_ref[...] = jnp.zeros_like(dwg_ref)
        dwu_ref[...] = jnp.zeros_like(dwu_ref)
        dwd_ref[...] = jnp.zeros_like(dwd_ref)

        def tn_dot(lhs, rhs):
            return lax.dot_general(lhs, rhs, (((0,), (0,)), ((), ())), preferred_element_type=F32)

        def chunk(step, carry):
            where_at, dy_parts = [], []
            for half in range(CHUNK):
                idx = list_ref[CHUNK * step + half]
                src, rng = idx // n_blk, pl.ds(pl.multiple_of((idx % n_blk) * BLK, BLK), BLK)
                where_at.append((src, rng))
                dy_part = dout_ref[src, 0, rng, :]
                dy_parts.append(jnp.where(CHUNK * step + half < count, dy_part, jnp.zeros_like(dy_part)))
            x_val = jnp.concatenate([row_ref[src, 0, rng, :] for src, rng in where_at], axis=0)
            dy_val = jnp.concatenate(dy_parts, axis=0)
            pre = jnp.dot(x_val, gu_ref[0], preferred_element_type=F32)
            d_act = jnp.dot(dy_val, dnt_ref[0], preferred_element_type=F32)
            gate_pre, up_pre = pre[:, :d_exp], pre[:, d_exp:]
            sig = jax.nn.sigmoid(gate_pre)
            gate_act = gate_pre * sig
            act = (gate_act * up_pre).astype(BF16)
            d_gate = (d_act * up_pre * (sig * (1.0 + gate_pre * (1.0 - sig)))).astype(BF16)
            d_up = (d_act * gate_act).astype(BF16)
            d_gu = jnp.concatenate([d_gate, d_up], axis=1)
            dx = jnp.dot(d_gu, gut_ref[0], preferred_element_type=F32).astype(BF16)
            dwd_ref[0] += tn_dot(act, dy_val)
            d_wgu = tn_dot(x_val, d_gu)
            dwg_ref[0] += d_wgu[:, :d_exp]
            dwu_ref[0] += d_wgu[:, d_exp:]
            for half, (src, rng) in enumerate(where_at):
                @pl.when(CHUNK * step + half < count)
                def _(half=half, src=src, rng=rng):
                    dx_ref[src, 0, rng, :] = dx[half * BLK:(half + 1) * BLK]
            return carry

        lax.fori_loop(0, (count + CHUNK - 1) // CHUNK, chunk, 0)

    row_spec = pl.BlockSpec((n_group, 1, n_cap, d_model), lambda e, f: (0, e, 0, 0))

    def mat_spec(n_in, n_out):
        return pl.BlockSpec((1, n_in, n_out), lambda e, f: (e, 0, 0))

    return pl.pallas_call(
        kernel,
        out_shape=(jax.ShapeDtypeStruct(rows.shape, BF16),
                   jax.ShapeDtypeStruct((n_exp, d_model, d_exp), F32),
                   jax.ShapeDtypeStruct((n_exp, d_model, d_exp), F32),
                   jax.ShapeDtypeStruct((n_exp, d_exp, d_model), F32)),
        grid_spec=pltpu.PrefetchScalarGridSpec(
            num_scalar_prefetch=1, grid=(n_exp,),
            in_specs=[row_spec, row_spec, mat_spec(d_model, 2 * d_exp), mat_spec(2 * d_exp, d_model), mat_spec(d_model, d_exp)],
            out_specs=(row_spec, mat_spec(d_model, d_exp), mat_spec(d_model, d_exp), mat_spec(d_exp, d_model)),
            scratch_shapes=[pltpu.SMEM((n_group * n_blk + 8,), jnp.int32)]),
        **compile_args(1.4 * n_group * n_exp * n_cap * d_model * d_exp * 8, n_group * n_exp * n_cap * d_model * 6),
    )(flags, rows, d_out, w_gu, w_gu_t, w_down_t)


def solution(mesh):
    n_stage = mesh.shape['pp']
    n_group = mesh.shape['ep']
    next_perm = [(stage_idx, (stage_idx + 1) % n_stage) for stage_idx in range(n_stage)]
    prev_perm = [(stage_idx, (stage_idx - 1) % n_stage) for stage_idx in range(n_stage)]
    def flip(bit):
        return [(dev, dev ^ bit) for dev in range(n_group)]

    def sources(flip_core):
        me = lax.axis_index('ep') ^ flip_core
        return me ^ (2 * jnp.arange(n_group // 2, dtype=jnp.int32))

    def wait_for(vals, after):
        return lax.optimization_barrier(tuple(vals) + tuple(after))[:len(vals)]

    class ReduceScatter:
        def __init__(self, combine, n_chunk, after):
            other_part = combine(sources(1), after)
            self.recv = lax.ppermute(other_part, 'ep', flip(1))
            self.part = combine(sources(0), (other_part,))
            n_tok, d_model = self.part.shape[1:]
            self.mid, self.size = d_model // 2, n_tok // n_chunk
            self.sends, self.recvs, self.lasts = [], [], [None] * n_chunk
            for chunk in range(n_chunk):
                if chunk:
                    self.part, self.recv = wait_for((self.part, self.recv), self.sends[-1])
                self.sends.append((jnp.stack([self.left(chunk, 1), self.left(chunk, 3)]), jnp.stack([self.right(chunk, 2), self.right(chunk, 3)])))
                x_send, y_send = wait_for(self.sends[-1], self.recvs[-1]) if chunk else self.sends[-1]
                self.recvs.append((lax.ppermute(x_send, 'ep', flip(2)), lax.ppermute(y_send, 'ep', flip(4))))

        def left(self, chunk, rel):
            rows = slice(chunk * self.size, (chunk + 1) * self.size)
            return self.part[rel, rows, :self.mid] + self.recv[rel, rows, :self.mid]

        def right(self, chunk, rel):
            rows = slice(chunk * self.size, (chunk + 1) * self.size)
            return self.part[rel, rows, self.mid:] + self.recv[rel, rows, self.mid:]

        def second(self, chunk, after):
            x_recv, y_recv = self.recvs[chunk] = wait_for(self.recvs[chunk], after)
            y_send, x_send = self.left(chunk, 2) + x_recv[1], self.right(chunk, 1) + y_recv[1]
            self.lasts[chunk] = (lax.ppermute(y_send, 'ep', flip(4)), lax.ppermute(x_send, 'ep', flip(2)))
            return y_send, x_send

        def final(self, chunk, after):
            x_recv, y_recv = self.recvs[chunk]
            y_last, x_last = wait_for(self.lasts[chunk], after)
            return jnp.concatenate([self.left(chunk, 0) + x_recv[0] + y_last, self.right(chunk, 0) + y_recv[0] + x_last], axis=1)

    class AllGather:
        def __init__(self, val):
            self.val, self.x_val, self.y_val = val, lax.ppermute(val, 'ep', flip(2)), lax.ppermute(val, 'ep', flip(4))

        def diagonal(self, after):
            self.x_val, self.y_val = wait_for((self.x_val, self.y_val), after)
            half = self.val.shape[0] // 2
            self.parts = (lax.ppermute(self.y_val[:half], 'ep', flip(2)), lax.ppermute(self.x_val[half:], 'ep', flip(4)))

        def finish(self, after):
            diag_val = jnp.concatenate(wait_for(self.parts, after), axis=0)
            mine = jnp.stack([self.val, self.x_val, self.y_val, diag_val])
            return mine, lax.ppermute(mine, 'ep', flip(1))

    tok_spec = P('pp', 'ep', None)
    rep_spec = P('pp', None, None)
    exp_spec = P('pp', 'ep', None, None)
    saved_spec = P('pp', None, 'ep', None, None)

    def slot_body(x_f, pos_f, gate_f, x_b, dy_b, pos_b, gate_b, xe_b, w_in, w_out, ws_gate, ws_up, ws_down, we_gate, we_up, we_down):
        x_f, pos_f, gate_f, x_b, dy_b, pos_b, gate_b, xe_b = x_f[0], pos_f[0], gate_f[0], x_b[0], dy_b[0], pos_b[0], gate_b[0], xe_b[0]
        w_in, w_out, ws_gate, ws_up, ws_down = w_in[0], w_out[0], ws_gate[0], ws_up[0], ws_down[0]
        we_gate, we_up, we_down = we_gate[0], we_up[0], we_down[0]
        n_tok, n_top = pos_f.shape
        d_model = x_f.shape[-1]
        n_exp = we_gate.shape[0]
        n_cap = xe_b.shape[2]
        n_rows = n_exp * n_cap // LANES
        buf_shape = (n_group, n_exp, n_cap, d_model)

        dy_gather = AllGather(dy_b)
        my_maps = route_maps(jnp.stack([pos_f.T, pos_b.T]), jnp.stack([gate_f.T, gate_b.T]).astype(F32), n_group, n_rows)
        maps = lax.all_to_all(my_maps, 'ep', 0, 0, tiled=True)
        maps = maps.reshape(n_group, 4, n_exp * n_cap // BLK, BLK)
        used = jnp.any(maps >= 0.0, axis=3).astype(jnp.int32)
        maps = jnp.concatenate([maps] * (LANES // BLK), axis=3)
        used_f, used_b = used[:, 0].reshape(-1), used[:, 2].reshape(-1)
        x_f, = wait_for((x_f,), (my_maps,))
        hidden, _, _ = dense_fwd(x_f, w_in, w_out)
        normed, _ = rms_norm(hidden)
        we_gate, we_up, we_down = wait_for((we_gate, we_up, we_down), (my_maps,))
        w_gu = jnp.concatenate([we_gate, we_up], axis=2)
        w_gu_t, w_down_t = (with_layout_constraint(w.transpose(0, 2, 1), Layout((0, 1, 2))) for w in (w_gu, we_down))
        dy_gather.diagonal((normed, w_gu_t, w_gu, w_down_t))
        x_b, = wait_for((x_b,), (dy_gather.x_val, dy_gather.y_val))
        hidden_b, inv_in, pre_act = dense_fwd(x_b, w_in, w_out)
        dy_mine, dy_other = dy_gather.finish((hidden_b,))
        z_gather = AllGather(wait_for((normed,), (hidden_b,))[0])

        d_rows = gather_rows(used_b, maps, 2, dy_mine, True, sources(0), ())
        d_rows = gather_rows(used_b, maps, 2, dy_other, True, sources(1), (), d_rows).reshape(buf_shape)
        z_gather.diagonal((d_rows,))
        d_rows, = wait_for((d_rows,), (z_gather.x_val, z_gather.y_val))
        dx_rows, d_wg, d_wu, d_wd = expert_back(used_b, xe_b, d_rows, w_gu, w_gu_t, w_down_t)
        dx_rows = dx_rows.reshape(n_group, n_exp * n_cap, d_model)
        d_sum = ReduceScatter(lambda srcs, after: combine_rows(used_b, maps, 2, dx_rows, n_tok, False, srcs, after), 1, z_gather.parts)
        z_mine, z_other = z_gather.finish((d_wg,))

        z_rows = gather_rows(used_f, maps, 0, z_mine, False, sources(0), d_sum.sends[0])
        z_rows = gather_rows(used_f, maps, 0, z_other, False, sources(1), (), z_rows).reshape(buf_shape)
        exp_out = expert_fwd(used_f, z_rows, w_gu, we_down).reshape(n_group, n_exp * n_cap, d_model)
        d_sends = d_sum.second(0, (exp_out,))
        y_sum = ReduceScatter(lambda srcs, after: combine_rows(used_f, maps, 0, exp_out, n_tok, True, srcs, after), 2, d_sends)
        y_started = y_sum.sends[0] + y_sum.sends[1]
        hidden_b, dy_b = wait_for((hidden_b, dy_b), y_started)
        normed_b, inv_mid = rms_norm(hidden_b)
        d_route = d_sum.final(0, y_started)
        d_norm = shared_back(normed_b, dy_b, ws_gate, ws_up, ws_down) + d_route
        d_hidden = dy_b.astype(F32) + rms_back(hidden_b, inv_mid, d_norm)
        size = n_tok // 2
        halves = [slice(i * size, (i + 1) * size) for i in range(2)]
        dx_parts = []
        for rows in halves:
            dx_parts.append(dense_back(d_hidden[rows], x_b[rows], inv_in[rows], pre_act[rows], w_in, w_out))
            if len(dx_parts) == 1:
                d_hidden, = wait_for((d_hidden,), y_sum.second(0, (dx_parts[0],)))
        dx_sent = [lax.ppermute(part, 'pp', prev_perm) for part in dx_parts]
        normed, = wait_for((normed,), (dx_parts[1],))
        shared = shared_fwd(normed, ws_gate, ws_up, ws_down)
        y_base = hidden.astype(F32) + shared
        y_parts, after = [], y_sum.second(1, (y_base, dx_sent[0]))
        for chunk, rows in enumerate(halves):
            y_parts.append((y_base[rows] + y_sum.final(chunk, after)).astype(BF16))
            after = (dx_sent[1], y_parts[0])
        y_sent = [lax.ppermute(part, 'pp', next_perm) for part in y_parts]
        y_next, dx_prev = jnp.concatenate(y_sent, axis=0), jnp.concatenate(dx_sent, axis=0)
        return y_next[None], dx_prev[None], d_wg[None], d_wu[None], d_wd[None]

    in_specs = (tok_spec,) * 7 + (saved_spec,) + (rep_spec,) * 5 + (exp_spec,) * 3
    out_specs = (tok_spec, tok_spec, exp_spec, exp_spec, exp_spec)
    return jax.shard_map(slot_body, mesh=mesh, in_specs=in_specs, out_specs=out_specs, check_vma=False)
```

```python
import functools

import jax
import jax.numpy as jnp
from jax import lax
from jax.experimental import pallas as pl
from jax.experimental.layout import Layout, with_layout_constraint
from jax.experimental.pallas import tpu as pltpu
from jax.sharding import PartitionSpec as P

EPS = 1e-6
LANES = 128
BLK = 64
CHUNK = 512 // BLK
F32 = jnp.float32
BF16 = jnp.bfloat16


def rms_norm(x_val):
    x_f32 = x_val.astype(F32)
    inv_rms = lax.rsqrt(jnp.mean(x_f32 * x_f32, axis=-1, keepdims=True) + EPS)
    return (x_f32 * inv_rms).astype(BF16), inv_rms


def rms_back(x_val, inv_rms, d_norm):
    x_f32 = x_val.astype(F32)
    proj_mean = jnp.mean(d_norm * x_f32, axis=-1, keepdims=True)
    return inv_rms * d_norm - x_f32 * (inv_rms * inv_rms * inv_rms) * proj_mean


def silu_grad(pre_val):
    sig_val = jax.nn.sigmoid(pre_val)
    return sig_val * (1.0 + pre_val * (1.0 - sig_val))


def dense_fwd(x_val, w_in, w_out):
    normed, inv_in = rms_norm(x_val)
    pre_act = jnp.dot(normed, w_in, preferred_element_type=F32)
    dense_act = jax.nn.silu(pre_act).astype(BF16)
    mlp_out = jnp.dot(dense_act, w_out, preferred_element_type=F32)
    return (x_val.astype(F32) + mlp_out).astype(BF16), inv_in, pre_act


def dense_back(d_hidden, x_val, inv_in, pre_act, w_in, w_out):
    d_act = jnp.einsum('th,fh->tf', d_hidden.astype(BF16), w_out, preferred_element_type=F32)
    d_pre = (d_act * silu_grad(pre_act)).astype(BF16)
    d_in = jnp.einsum('tf,hf->th', d_pre, w_in, preferred_element_type=F32)
    return (d_hidden + rms_back(x_val, inv_in, d_in)).astype(BF16)


def shared_fwd(normed, ws_gate, ws_up, ws_down):
    gate_pre = jnp.dot(normed, ws_gate, preferred_element_type=F32)
    up_pre = jnp.dot(normed, ws_up, preferred_element_type=F32)
    glu_act = (jax.nn.silu(gate_pre) * up_pre).astype(BF16)
    return jnp.dot(glu_act, ws_down, preferred_element_type=F32)


def shared_back(normed, d_out, ws_gate, ws_up, ws_down):
    gate_pre = jnp.dot(normed, ws_gate, preferred_element_type=F32)
    up_pre = jnp.dot(normed, ws_up, preferred_element_type=F32)
    d_act = jnp.einsum('th,fh->tf', d_out, ws_down, preferred_element_type=F32)
    d_gate = (d_act * up_pre * silu_grad(gate_pre)).astype(BF16)
    d_up = (d_act * jax.nn.silu(gate_pre)).astype(BF16)
    return jnp.einsum('tf,hf->th', d_gate, ws_gate, preferred_element_type=F32) + jnp.einsum('tf,hf->th', d_up, ws_up, preferred_element_type=F32)


def iota_f32(shape, dim):
    return lax.broadcasted_iota(jnp.int32, shape, dim).astype(F32)


def compile_args(flops, n_bytes, vmem_mib=56):
    return dict(
        compiler_params=pltpu.CompilerParams(
            dimension_semantics=('arbitrary',), vmem_limit_bytes=vmem_mib * 1024 * 1024),
        cost_estimate=pl.CostEstimate(flops=int(flops), bytes_accessed=int(n_bytes), transcendentals=0))


def route_maps(pos_pair, gate_pair, n_group, n_rows):
    n_set, n_top, n_tok = pos_pair.shape
    n_hi = n_group * n_rows

    def kernel(pos_ref, gate_ref, out_ref):
        tok_row = lax.broadcasted_iota(jnp.int32, (1, n_tok), 1) + 1
        tok_hi = (tok_row >> 6).astype(F32)
        tok_lo = (tok_row & 63).astype(F32)
        hi_iota = lax.broadcasted_iota(jnp.int32, (n_hi, n_tok), 0)
        lo_iota = lax.broadcasted_iota(jnp.int32, (LANES, n_tok), 0)
        for set_idx in range(n_set):
            def add_route(rank, total):
                pos_row = pos_ref[set_idx, pl.ds(rank, 1), :]
                gate_row = gate_ref[set_idx, pl.ds(rank, 1), :]
                hi_hot = jnp.where(hi_iota == (pos_row >> 7), 1.0, 0.0).astype(BF16)
                lo_eq = lo_iota == (pos_row & (LANES - 1))
                rhs = jnp.concatenate([jnp.where(lo_eq, val, 0.0).astype(BF16) for val in (tok_hi, tok_lo, gate_row)], axis=0)
                return total + lax.dot_general(hi_hot, rhs, (((1,), (1,)), ((), ())), preferred_element_type=F32)

            total = lax.fori_loop(0, n_top, add_route, jnp.zeros((n_hi, 3 * LANES), F32))
            tok_map = total[:, :LANES] * 64.0 + total[:, LANES:2 * LANES] - 1.0
            out_ref[:, 2 * set_idx] = tok_map.reshape(n_group, n_rows, LANES)
            out_ref[:, 2 * set_idx + 1] = total[:, 2 * LANES:].reshape(n_group, n_rows, LANES)

    return pl.pallas_call(
        kernel,
        out_shape=jax.ShapeDtypeStruct((n_group, 2 * n_set, n_rows, LANES), F32),
        compiler_params=pltpu.CompilerParams(vmem_limit_bytes=48 * 1024 * 1024),
        cost_estimate=pl.CostEstimate(flops=2 * n_set * n_top * n_tok * n_hi * 3 * LANES, bytes_accessed=2 ** 20, transcendentals=0),
    )(pos_pair, gate_pair)


def list_blocks(flag_at, list_ref, n_rows, pad_to):
    def step(idx, count):
        list_ref[count] = idx
        return count + flag_at(idx)

    count = lax.fori_loop(0, n_rows, step, jnp.int32(0))
    last = list_ref[jnp.maximum(count - 1, 0)]
    for extra in range(pad_to - 1):
        list_ref[count + extra] = last
    return count


def run_chunks(count, chunk):
    n_full = (count + CHUNK // 2 - 1) // CHUNK
    lax.fori_loop(0, n_full, functools.partial(chunk, CHUNK, 0), 0)
    base = n_full * CHUNK
    lax.fori_loop(0, (count > base).astype(jnp.int32), functools.partial(chunk, CHUNK // 2, base), 0)


def gather_rows(flags, maps, tok_plane, rows, gated, sources, after, into=None):
    n_group, n_rows = maps.shape[0], maps.shape[2]
    n_src, n_tok, d_model = rows.shape
    n_slots = n_rows * BLK
    extra = tuple(after) + (() if into is None else (into,))

    def kernel(flag_ref, source_ref, tok_ref, gate_ref, row_ref, *refs):
        out_ref, list_ref = refs[-2:]
        src = source_ref[pl.program_id(0)]
        count = list_blocks(lambda idx: flag_ref[src * n_rows + idx], list_ref, n_rows, CHUNK)
        lane = iota_f32((BLK, LANES), 1)

        def columns(ref, idx):
            return jnp.transpose(jnp.broadcast_to(ref[0, 0, pl.ds(idx, 1), :], (LANES, LANES)))[:BLK]

        def chunk(n_part, base, step, carry):
            picks = []
            for entry in range(n_part):
                idx = list_ref[base + n_part * step + entry]
                tok_col = columns(tok_ref, idx)
                tok_hi = jnp.floor(tok_col * (1.0 / LANES))
                val = columns(gate_ref, idx) if gated else 1.0
                hot = jnp.where(tok_col - tok_hi * LANES == lane, val, 0.0).astype(BF16)
                tok_hi = tok_hi.astype(BF16)
                picks.append(jnp.concatenate(
                    [jnp.where(tok_hi == jnp.asarray(part, BF16), hot, jnp.zeros_like(hot)) for part in range(n_tok // LANES)], axis=1))
            picked = jnp.dot(jnp.concatenate(picks, axis=0), row_ref[0], preferred_element_type=F32).astype(BF16)
            for entry in range(n_part):
                idx = list_ref[base + n_part * step + entry]
                out_ref[0, pl.ds(pl.multiple_of(idx * BLK, BLK), BLK), :] = picked[entry * BLK:(entry + 1) * BLK]
            return carry

        run_chunks(count, chunk)

    return pl.pallas_call(
        kernel,
        out_shape=jax.ShapeDtypeStruct((n_group, n_slots, d_model), BF16),
        grid_spec=pltpu.PrefetchScalarGridSpec(
            num_scalar_prefetch=2, grid=(n_src,),
            in_specs=[
                pl.BlockSpec((1, 1, n_rows, LANES), lambda s, f, o: (o[s], tok_plane, 0, 0)),
                pl.BlockSpec((1, 1, n_rows, LANES), lambda s, f, o: (o[s], tok_plane + 1, 0, 0)),
                pl.BlockSpec((1, n_tok, d_model), lambda s, f, o: (s, 0, 0)),
            ] + [pl.BlockSpec(memory_space=pl.ANY)] * len(extra),
            out_specs=pl.BlockSpec((1, n_slots, d_model), lambda s, f, o: (o[s], 0, 0)),
            scratch_shapes=[pltpu.SMEM((n_rows + 8,), jnp.int32)]),
        input_output_aliases={} if into is None else {4 + len(extra): 0},
        **compile_args(1.2 * n_src * n_slots * n_tok * d_model, n_src * (n_slots + n_tok) * d_model * 2),
    )(flags, sources, maps, maps, rows, *extra)


def combine_rows(flags, maps, tok_plane, rows, n_tok, gated, sources, after):
    n_group = sources.shape[0]
    n_slots, d_model = rows.shape[1:]
    n_rows = maps.shape[2]
    m_tile = 1024

    def kernel(flag_ref, source_ref, tok_ref, gate_ref, row_ref, *refs):
        out_ref, list_ref = refs[-2:]
        src = source_ref[pl.program_id(0)]
        count = list_blocks(lambda idx: flag_ref[src * n_rows + idx], list_ref, n_rows, CHUNK)
        out_ref[...] = jnp.zeros_like(out_ref)
        tok_iota = iota_f32((LANES, LANES), 0)
        low_lanes = lax.broadcasted_iota(jnp.int32, (1, LANES), 1) < BLK

        def chunk(n_part, base, step, carry):
            toks, vals, parts = [], [], []
            for entry in range(n_part):
                idx = list_ref[base + n_part * step + entry]
                toks.append(jnp.where(base + n_part * step + entry < count, tok_ref[0, 0, pl.ds(idx, 1), :], -1.0))
                vals.append(gate_ref[0, 0, pl.ds(idx, 1), :] if gated else 1.0)
                parts.append(row_ref[0, pl.ds(pl.multiple_of(idx * BLK, BLK), BLK), :])
            toks = [jnp.where(low_lanes, *toks[2 * part:2 * part + 2]) for part in range(n_part // 2)]
            hots, his = [], []
            for part in range(n_part // 2):
                val = jnp.where(low_lanes, *vals[2 * part:2 * part + 2]) if gated else 1.0
                tok_hi = jnp.floor(toks[part] * (1.0 / LANES))
                hots.append(jnp.where(tok_iota == toks[part] - tok_hi * LANES, val, 0.0).astype(BF16))
                his.append(jnp.broadcast_to(tok_hi, (LANES, LANES)).astype(BF16))
            row_chunk = jnp.concatenate(parts, axis=0)
            for m_idx in range(n_tok // m_tile):
                weights = jnp.concatenate([jnp.concatenate(
                    [jnp.where(hi == jnp.asarray(sub, BF16), hot, jnp.zeros_like(hot)) for sub in range(m_idx * m_tile // LANES, (m_idx + 1) * m_tile // LANES)],
                    axis=0) for hot, hi in zip(hots, his)], axis=1)
                out_ref[0, m_idx * m_tile:(m_idx + 1) * m_tile, :] += jnp.dot(weights, row_chunk, preferred_element_type=F32)
            return carry

        run_chunks(count, chunk)

    return pl.pallas_call(
        kernel,
        out_shape=jax.ShapeDtypeStruct((n_group, n_tok, d_model), F32),
        grid_spec=pltpu.PrefetchScalarGridSpec(
            num_scalar_prefetch=2, grid=(n_group,),
            in_specs=[
                pl.BlockSpec((1, 1, n_rows, LANES), lambda s, f, o: (o[s], tok_plane, 0, 0)),
                pl.BlockSpec((1, 1, n_rows, LANES), lambda s, f, o: (o[s], tok_plane + 1, 0, 0)),
                pl.BlockSpec((1, n_slots, d_model), lambda s, f, o: (o[s], 0, 0)),
            ] + [pl.BlockSpec(memory_space=pl.ANY)] * len(after),
            out_specs=pl.BlockSpec((1, n_tok, d_model), lambda s, f, o: (s, 0, 0)),
            scratch_shapes=[pltpu.SMEM((n_rows + 8,), jnp.int32)]),
        **compile_args(1.2 * n_group * n_slots * n_tok * d_model, n_group * (n_slots * 2 + n_tok * 4) * d_model),
    )(flags, sources, maps, maps, rows, *after)


def expert_fwd(flags, rows, w_gu, w_down):
    n_group, n_exp, n_cap, d_model = rows.shape
    d_exp = w_down.shape[1]
    n_blk = n_cap // BLK
    n_rows = n_exp * n_blk

    def kernel(flag_ref, row_ref, gu_ref, down_ref, out_ref, list_ref):
        exp_idx = pl.program_id(0)
        flag_at = lambda idx: flag_ref[(idx // n_blk) * n_rows + exp_idx * n_blk + idx % n_blk]
        count = list_blocks(flag_at, list_ref, n_group * n_blk, CHUNK)

        def chunk(n_part, base, step, carry):
            where_at = []
            for half in range(n_part):
                idx = list_ref[base + n_part * step + half]
                where_at.append((idx // n_blk, pl.ds(pl.multiple_of((idx % n_blk) * BLK, BLK), BLK)))
            x_val = jnp.concatenate([row_ref[s, 0, rng, :] for s, rng in where_at], axis=0)
            pre = jnp.dot(x_val, gu_ref[0], preferred_element_type=F32)
            act = (jax.nn.silu(pre[:, :d_exp]) * pre[:, d_exp:]).astype(BF16)
            out = jnp.dot(act, down_ref[0], preferred_element_type=F32).astype(BF16)
            for half, (s, rng) in enumerate(where_at):
                out_ref[s, 0, rng, :] = out[half * BLK:(half + 1) * BLK]
            return carry

        run_chunks(count, chunk)

    row_spec = pl.BlockSpec((n_group, 1, n_cap, d_model), lambda e, f: (0, e, 0, 0))
    return pl.pallas_call(
        kernel,
        out_shape=jax.ShapeDtypeStruct(rows.shape, BF16),
        grid_spec=pltpu.PrefetchScalarGridSpec(
            num_scalar_prefetch=1, grid=(n_exp,),
            in_specs=[row_spec,
                      pl.BlockSpec((1, d_model, 2 * d_exp), lambda e, f: (e, 0, 0)),
                      pl.BlockSpec((1, d_exp, d_model), lambda e, f: (e, 0, 0))],
            out_specs=row_spec,
            scratch_shapes=[pltpu.SMEM((n_group * n_blk + 8,), jnp.int32)]),
        **compile_args(1.4 * n_group * n_exp * n_cap * d_model * d_exp * 3, n_group * n_exp * n_cap * d_model * 4),
    )(flags, rows, w_gu, w_down)


def expert_back(flags, rows, d_out, w_gu, w_gu_t, w_down_t):
    n_group, n_exp, n_cap, d_model = rows.shape
    d_exp = w_down_t.shape[2]
    n_blk = n_cap // BLK
    n_rows = n_exp * n_blk

    def kernel(flag_ref, row_ref, dout_ref, gu_ref, gut_ref, dnt_ref, dx_ref, dwg_ref, dwu_ref, dwd_ref, list_ref):
        exp_idx = pl.program_id(0)
        flag_at = lambda idx: flag_ref[(idx // n_blk) * n_rows + exp_idx * n_blk + idx % n_blk]
        count = list_blocks(flag_at, list_ref, n_group * n_blk, CHUNK)
        dwg_ref[...] = jnp.zeros_like(dwg_ref)
        dwu_ref[...] = jnp.zeros_like(dwu_ref)
        dwd_ref[...] = jnp.zeros_like(dwd_ref)

        def tn_dot(lhs, rhs):
            return lax.dot_general(lhs, rhs, (((0,), (0,)), ((), ())), preferred_element_type=F32)

        def chunk(n_part, base, step, carry):
            where_at, dy_parts = [], []
            for half in range(n_part):
                idx = list_ref[base + n_part * step + half]
                src, rng = idx // n_blk, pl.ds(pl.multiple_of((idx % n_blk) * BLK, BLK), BLK)
                where_at.append((src, rng))
                dy_part = dout_ref[src, 0, rng, :]
                dy_parts.append(jnp.where(base + n_part * step + half < count, dy_part, jnp.zeros_like(dy_part)))
            x_val = jnp.concatenate([row_ref[src, 0, rng, :] for src, rng in where_at], axis=0)
            dy_val = jnp.concatenate(dy_parts, axis=0)
            pre = jnp.dot(x_val, gu_ref[0], preferred_element_type=F32)
            d_act = jnp.dot(dy_val, dnt_ref[0], preferred_element_type=F32)
            gate_pre, up_pre = pre[:, :d_exp], pre[:, d_exp:]
            sig = jax.nn.sigmoid(gate_pre)
            gate_act = gate_pre * sig
            act = (gate_act * up_pre).astype(BF16)
            d_gate = (d_act * up_pre * (sig * (1.0 + gate_pre * (1.0 - sig)))).astype(BF16)
            d_up = (d_act * gate_act).astype(BF16)
            d_gu = jnp.concatenate([d_gate, d_up], axis=1)
            dx = jnp.dot(d_gu, gut_ref[0], preferred_element_type=F32).astype(BF16)
            dwd_ref[0] += tn_dot(act, dy_val)
            d_wgu = tn_dot(x_val, d_gu)
            dwg_ref[0] += d_wgu[:, :d_exp]
            dwu_ref[0] += d_wgu[:, d_exp:]
            for half, (src, rng) in enumerate(where_at):
                @pl.when(base + n_part * step + half < count)
                def _(half=half, src=src, rng=rng):
                    dx_ref[src, 0, rng, :] = dx[half * BLK:(half + 1) * BLK]
            return carry

        run_chunks(count, chunk)

    row_spec = pl.BlockSpec((n_group, 1, n_cap, d_model), lambda e, f: (0, e, 0, 0))

    def mat_spec(n_in, n_out):
        return pl.BlockSpec((1, n_in, n_out), lambda e, f: (e, 0, 0))

    return pl.pallas_call(
        kernel,
        out_shape=(jax.ShapeDtypeStruct(rows.shape, BF16),
                   jax.ShapeDtypeStruct((n_exp, d_model, d_exp), F32),
                   jax.ShapeDtypeStruct((n_exp, d_model, d_exp), F32),
                   jax.ShapeDtypeStruct((n_exp, d_exp, d_model), F32)),
        grid_spec=pltpu.PrefetchScalarGridSpec(
            num_scalar_prefetch=1, grid=(n_exp,),
            in_specs=[row_spec, row_spec, mat_spec(d_model, 2 * d_exp), mat_spec(2 * d_exp, d_model), mat_spec(d_model, d_exp)],
            out_specs=(row_spec, mat_spec(d_model, d_exp), mat_spec(d_model, d_exp), mat_spec(d_exp, d_model)),
            scratch_shapes=[pltpu.SMEM((n_group * n_blk + 8,), jnp.int32)]),
        **compile_args(1.4 * n_group * n_exp * n_cap * d_model * d_exp * 8, n_group * n_exp * n_cap * d_model * 6),
    )(flags, rows, d_out, w_gu, w_gu_t, w_down_t)


def solution(mesh):
    n_stage = mesh.shape['pp']
    n_group = mesh.shape['ep']
    next_perm = [(stage_idx, (stage_idx + 1) % n_stage) for stage_idx in range(n_stage)]
    prev_perm = [(stage_idx, (stage_idx - 1) % n_stage) for stage_idx in range(n_stage)]
    def flip(bit):
        return [(dev, dev ^ bit) for dev in range(n_group)]

    def sources(flip_core):
        me = lax.axis_index('ep') ^ flip_core
        return me ^ (2 * jnp.arange(n_group // 2, dtype=jnp.int32))

    def wait_for(vals, after):
        return lax.optimization_barrier(tuple(vals) + tuple(after))[:len(vals)]

    class ReduceScatter:
        def __init__(self, combine, n_chunk, after):
            other_part = combine(sources(1), after)
            self.recv = lax.ppermute(other_part, 'ep', flip(1))
            self.part = combine(sources(0), (other_part,))
            n_tok, d_model = self.part.shape[1:]
            self.mid, self.size = d_model // 2, n_tok // n_chunk
            self.sends, self.recvs, self.lasts = [], [], [None] * n_chunk
            for chunk in range(n_chunk):
                if chunk:
                    self.part, self.recv = wait_for((self.part, self.recv), self.sends[-1])
                self.sends.append((jnp.stack([self.left(chunk, 1), self.left(chunk, 3)]), jnp.stack([self.right(chunk, 2), self.right(chunk, 3)])))
                x_send, y_send = self.sends[-1]
                self.recvs.append((lax.ppermute(x_send, 'ep', flip(2)), lax.ppermute(y_send, 'ep', flip(4))))

        def left(self, chunk, rel):
            rows = slice(chunk * self.size, (chunk + 1) * self.size)
            return self.part[rel, rows, :self.mid] + self.recv[rel, rows, :self.mid]

        def right(self, chunk, rel):
            rows = slice(chunk * self.size, (chunk + 1) * self.size)
            return self.part[rel, rows, self.mid:] + self.recv[rel, rows, self.mid:]

        def second(self, chunk, after):
            x_recv, y_recv = self.recvs[chunk] = wait_for(self.recvs[chunk], after)
            y_send, x_send = self.left(chunk, 2) + x_recv[1], self.right(chunk, 1) + y_recv[1]
            self.lasts[chunk] = (lax.ppermute(y_send, 'ep', flip(4)), lax.ppermute(x_send, 'ep', flip(2)))
            return y_send, x_send

        def final(self, chunk, after):
            x_recv, y_recv = self.recvs[chunk]
            y_last, x_last = wait_for(self.lasts[chunk], after)
            return jnp.concatenate([self.left(chunk, 0) + x_recv[0] + y_last, self.right(chunk, 0) + y_recv[0] + x_last], axis=1)

    class AllGather:
        def __init__(self, val):
            self.val, self.x_val, self.y_val = val, lax.ppermute(val, 'ep', flip(2)), lax.ppermute(val, 'ep', flip(4))

        def diagonal(self, after):
            self.x_val, self.y_val = wait_for((self.x_val, self.y_val), after)
            half = self.val.shape[0] // 2
            self.parts = (lax.ppermute(self.y_val[:half], 'ep', flip(2)), lax.ppermute(self.x_val[half:], 'ep', flip(4)))

        def finish(self, after):
            diag_val = jnp.concatenate(wait_for(self.parts, after), axis=0)
            mine = jnp.stack([self.val, self.x_val, self.y_val, diag_val])
            return mine, lax.ppermute(mine, 'ep', flip(1))

    tok_spec = P('pp', 'ep', None)
    rep_spec = P('pp', None, None)
    exp_spec = P('pp', 'ep', None, None)
    saved_spec = P('pp', None, 'ep', None, None)

    def slot_body(x_f, pos_f, gate_f, x_b, dy_b, pos_b, gate_b, xe_b, w_in, w_out, ws_gate, ws_up, ws_down, we_gate, we_up, we_down):
        x_f, pos_f, gate_f, x_b, dy_b, pos_b, gate_b, xe_b = x_f[0], pos_f[0], gate_f[0], x_b[0], dy_b[0], pos_b[0], gate_b[0], xe_b[0]
        w_in, w_out, ws_gate, ws_up, ws_down = w_in[0], w_out[0], ws_gate[0], ws_up[0], ws_down[0]
        we_gate, we_up, we_down = we_gate[0], we_up[0], we_down[0]
        n_tok, n_top = pos_f.shape
        d_model = x_f.shape[-1]
        n_exp = we_gate.shape[0]
        n_cap = xe_b.shape[2]
        n_rows = n_exp * n_cap // LANES
        buf_shape = (n_group, n_exp, n_cap, d_model)

        dy_gather = AllGather(dy_b)
        my_maps = route_maps(jnp.stack([pos_f.T, pos_b.T]), jnp.stack([gate_f.T, gate_b.T]).astype(F32), n_group, n_rows)
        maps = lax.all_to_all(my_maps, 'ep', 0, 0, tiled=True)
        maps = maps.reshape(n_group, 4, n_exp * n_cap // BLK, BLK)
        used = jnp.any(maps >= 0.0, axis=3).astype(jnp.int32)
        maps = jnp.concatenate([maps] * (LANES // BLK), axis=3)
        used_f, used_b = used[:, 0].reshape(-1), used[:, 2].reshape(-1)
        x_f, = wait_for((x_f,), (my_maps,))
        hidden, _, _ = dense_fwd(x_f, w_in, w_out)
        normed, _ = rms_norm(hidden)
        we_gate, we_up, we_down = wait_for((we_gate, we_up, we_down), (my_maps,))
        w_gu = jnp.concatenate([we_gate, we_up], axis=2)
        w_gu_t, w_down_t = (with_layout_constraint(w.transpose(0, 2, 1), Layout((0, 1, 2))) for w in (w_gu, we_down))
        dy_gather.diagonal((normed, w_gu_t, w_gu, w_down_t))
        x_b, = wait_for((x_b,), (dy_gather.x_val, dy_gather.y_val, maps, used_b, used_f))
        hidden_b, inv_in, pre_act = dense_fwd(x_b, w_in, w_out)
        dy_mine, dy_other = dy_gather.finish((hidden_b,))
        z_gather = AllGather(wait_for((normed,), (hidden_b,))[0])

        d_rows = gather_rows(used_b, maps, 2, dy_mine, True, sources(0), ())
        d_rows = gather_rows(used_b, maps, 2, dy_other, True, sources(1), (), d_rows).reshape(buf_shape)
        z_gather.diagonal((d_rows,))
        d_rows, = wait_for((d_rows,), (z_gather.x_val, z_gather.y_val))
        dx_rows, d_wg, d_wu, d_wd = expert_back(used_b, xe_b, d_rows, w_gu, w_gu_t, w_down_t)
        dx_rows = dx_rows.reshape(n_group, n_exp * n_cap, d_model)
        d_sum = ReduceScatter(lambda srcs, after: combine_rows(used_b, maps, 2, dx_rows, n_tok, False, srcs, after), 1, z_gather.parts)
        z_mine, z_other = z_gather.finish((d_wg,))

        z_rows = gather_rows(used_f, maps, 0, z_mine, False, sources(0), d_sum.sends[0])
        z_rows = gather_rows(used_f, maps, 0, z_other, False, sources(1), (), z_rows).reshape(buf_shape)
        exp_out = expert_fwd(used_f, z_rows, w_gu, we_down).reshape(n_group, n_exp * n_cap, d_model)
        d_sends = d_sum.second(0, (exp_out,))
        y_sum = ReduceScatter(lambda srcs, after: combine_rows(used_f, maps, 0, exp_out, n_tok, True, srcs, after), 2, d_sends)
        y_started = y_sum.sends[0] + y_sum.sends[1]
        hidden_b, dy_b = wait_for((hidden_b, dy_b), y_started)
        normed_b, inv_mid = rms_norm(hidden_b)
        d_route = d_sum.final(0, y_started)
        d_norm = shared_back(normed_b, dy_b, ws_gate, ws_up, ws_down) + d_route
        d_hidden = dy_b.astype(F32) + rms_back(hidden_b, inv_mid, d_norm)
        size = n_tok // 2
        halves = [slice(i * size, (i + 1) * size) for i in range(2)]
        dx_parts = []
        for rows in halves:
            dx_parts.append(dense_back(d_hidden[rows], x_b[rows], inv_in[rows], pre_act[rows], w_in, w_out))
            if len(dx_parts) == 1:
                d_hidden, = wait_for((d_hidden,), y_sum.second(0, (dx_parts[0],)))
        dx_sent = [lax.ppermute(part, 'pp', prev_perm) for part in dx_parts]
        normed, = wait_for((normed,), (dx_parts[1],))
        shared = shared_fwd(normed, ws_gate, ws_up, ws_down)
        y_base = hidden.astype(F32) + shared
        y_sent, after = [], y_sum.second(1, (y_base, dx_sent[0]))
        for chunk, rows in enumerate(halves):
            y_part = (y_base[rows] + y_sum.final(chunk, after)).astype(BF16)
            y_sent.append(lax.ppermute(y_part, 'pp', next_perm))
            after = (dx_sent[1], y_sent[0])
        y_next, dx_prev = jnp.concatenate(y_sent, axis=0), jnp.concatenate(dx_sent, axis=0)
        return y_next[None], dx_prev[None], d_wg[None], d_wu[None], d_wd[None]

    in_specs = (tok_spec,) * 7 + (saved_spec,) + (rep_spec,) * 5 + (exp_spec,) * 3
    out_specs = (tok_spec, tok_spec, exp_spec, exp_spec, exp_spec)
    return jax.shard_map(slot_body, mesh=mesh, in_specs=in_specs, out_specs=out_specs, check_vma=False)
```
